32 devices in a mesh: clip: 4 (over y, x), head: 8 (over z, core).
Axes of the slice: x: 2, y: 2, z: 4, core: 2. Of those that a mesh axis runs over, the one named last changes fastest.
Arguments:
- queries: bfloat16 [8192, 4096], P(('clip', 'head')), may hold values from -6 to 6
- key_rows: bfloat16 [8192, 4096], P(('clip', 'head')), may hold values from -6 to 6
- value_rows: bfloat16 [8192, 4096], P(('clip', 'head')), may hold values from -6 to 6
- query_tangent: bfloat16 [8192, 4096], P(('clip', 'head')), may hold values from -6 to 6
- key_tangent: bfloat16 [8192, 4096], P(('clip', 'head')), may hold values from -6 to 6
- value_tangent: bfloat16 [8192, 4096], P(('clip', 'head')), may hold values from -6 to 6
- partners: int32 [8, 2], replicated, may hold values from 0 to 7, as said below
- cotangent: bfloat16 [8192, 3072], P('clip'), may hold values from -6 to 6
Outputs:
- attended: bfloat16 [8192, 4096], P(('clip', 'head'))
- attended_tangent: bfloat16 [8192, 4096], P(('clip', 'head'))
- weight_grad: float32 [3072, 4096], P('clip', 'head')
The draws below stay inside these ranges and needn't reach their ends.
Inputs may be any that keep to these rules, and one draw needn't show every extreme that they name: `partners`: for clip c the two entries are distinct clips (c - d) mod 8 with 1 <= d <= 2 + c % 2.
All inputs are finite; a program needn't handle non-finite values.
Results may differ from the reference program's by a relative error of at most 0.0051.
Values may be sent and summed in bfloat16 or wider, within the bound.
A program may use at most 192 MiB of HBM per device.

```python
import jax
import jax.numpy as jnp
from jax import lax

HEADS = 32
HDIM = 128
DOUT = 3072
CLIP = 1024
CLIPS_DEV = 2
CLIPS = 8
TOKENS = 8192
QW = 4096


def shared_rows(key):
    base_q = jnp.clip(jax.random.normal(jax.random.fold_in(key, 11), (TOKENS, QW), jnp.float32), -6.0, 6.0)
    base_k = jnp.clip(jax.random.normal(jax.random.fold_in(key, 12), (TOKENS, QW), jnp.float32), -6.0, 6.0)
    return (base_q, base_k)


def draw_queries(key, part):
    return shared_rows(key)[0].astype(jnp.bfloat16)


def draw_key_rows(key, part):
    return shared_rows(key)[1].astype(jnp.bfloat16)


def draw_partners(key, part):
    clip_ids = jnp.arange(CLIPS, dtype=jnp.int32)
    gap_reach = CLIPS_DEV + clip_ids % CLIPS_DEV
    first_gap = jax.random.randint(jax.random.fold_in(key, 21), (CLIPS,), 0, 1 << 20) % gap_reach + 1
    gap_step = jax.random.randint(jax.random.fold_in(key, 22), (CLIPS,), 0, 1 << 20) % (gap_reach - 1) + 1
    second_gap = (first_gap - 1 + gap_step) % gap_reach + 1
    return jnp.stack([(clip_ids - first_gap) % CLIPS, (clip_ids - second_gap) % CLIPS], axis=1).astype(jnp.int32)


def spiked(result, key, source, target, shards_of, factor):
    def block_of(axis_at):
        return (jnp.arange(result.shape[axis_at]) // (result.shape[axis_at] // shards_of)).reshape((-1,) + (1,) * (result.ndim - 1 - axis_at))

    near = jax.random.permutation(key, shards_of)[block_of(target)]
    other_side = (block_of(target) + shards_of // 2) % shards_of
    return jnp.where((block_of(source) == near) | (block_of(source) == other_side), factor * result, result)


def steps_of(key, shape, shards, smallest, top_value):
    loudness = 1.0
    for dim, parts in shards:
        draws = jax.random.uniform(jax.random.fold_in(jax.random.fold_in(key, 6), dim), (parts,), jnp.float32, smallest / len(shards), top_value / len(shards))
        loudness = loudness * jnp.repeat(jnp.exp(draws), shape[dim] // parts).reshape((-1,) + (1,) * (len(shape) - 1 - dim))
    return loudness


def gaussian(stream_key, dims, width, limit, split=(), kind=jnp.bfloat16):
    entries = width * jax.random.normal(stream_key, dims, jnp.float32)
    if split:
        entries = entries * steps_of(stream_key, dims, split, -0.22, 0.18)
    return jnp.clip(entries, -limit, limit).astype(kind)


def bell_draw_with(own_key, extent, width, reach, cuts, heavy, kind=jnp.bfloat16):
    result = width * jax.random.normal(own_key, extent, jnp.float32)
    if cuts:
        result = result * steps_of(own_key, extent, cuts, -0.22, 0.18)
    return jnp.clip(spiked(result, jax.random.fold_in(own_key, 3), *heavy), -reach, reach).astype(kind)


def setup_inputs(seed: int = 0) -> dict:
    arg_keys = jax.random.split(jax.random.key(seed), 9)
    queries = draw_queries(jax.random.fold_in(arg_keys[8], 71), 0)
    key_rows = draw_key_rows(jax.random.fold_in(arg_keys[8], 71), 0)
    value_rows = gaussian(arg_keys[2], (TOKENS, QW), 1.0, 6.0, ((0, 32),))
    query_tangent = gaussian(arg_keys[3], (TOKENS, QW), 1.0, 6.0, ((0, 32),))
    key_tangent = gaussian(arg_keys[4], (TOKENS, QW), 1.0, 6.0, ((0, 32),))
    value_tangent = gaussian(arg_keys[5], (TOKENS, QW), 1.0, 6.0, ((0, 32),))
    partners = draw_partners(jax.random.fold_in(arg_keys[8], 71), 0)
    cotangent = bell_draw_with(arg_keys[7], (TOKENS, DOUT), 1.0, 6.0, ((0, 4),), (0, 1, 4, 2.0))
    return dict(queries=queries, key_rows=key_rows, value_rows=value_rows, query_tangent=query_tangent, key_tangent=key_tangent, value_tangent=value_tangent, partners=partners, cotangent=cotangent)


def attend_head(query_part, qtan_part, key_win, value_win, ktan_win, vtan_win):
    score_scale = HDIM ** -0.5
    scores = jnp.dot(query_part, key_win.T, preferred_element_type=jnp.float32) * score_scale
    score_tan = (jnp.dot(qtan_part, key_win.T, preferred_element_type=jnp.float32)
                 + jnp.dot(query_part, ktan_win.T, preferred_element_type=jnp.float32)) * score_scale
    row_max = jnp.max(scores, axis=-1, keepdims=True)
    raw_weights = jnp.exp(scores - row_max)
    row_total = jnp.sum(raw_weights, axis=-1, keepdims=True)
    probability = raw_weights / row_total
    tangent_mean = jnp.sum(probability * score_tan, axis=-1, keepdims=True)
    prob_tangent = probability * (score_tan - tangent_mean)
    prob_low = probability.astype(jnp.bfloat16)
    tangent_low = prob_tangent.astype(jnp.bfloat16)
    result_out = jnp.dot(prob_low, value_win, preferred_element_type=jnp.float32)
    tangent_out = (jnp.dot(tangent_low, value_win, preferred_element_type=jnp.float32)
                   + jnp.dot(prob_low, vtan_win, preferred_element_type=jnp.float32))
    return result_out.astype(jnp.bfloat16), tangent_out.astype(jnp.bfloat16)


def reference(queries, key_rows, value_rows, query_tangent, key_tangent, value_tangent, partners, cotangent):
    def split_heads(array):
        return array.reshape(CLIPS, CLIP, HEADS, HDIM)

    queries4 = split_heads(queries)
    keys4 = split_heads(key_rows)
    values4 = split_heads(value_rows)
    qtan4 = split_heads(query_tangent)
    ktan4 = split_heads(key_tangent)
    vtan4 = split_heads(value_tangent)

    def one_clip(clip_index):
        partner_row = partners[clip_index]
        chosen = jnp.stack([clip_index, partner_row[0], partner_row[1]]).astype(jnp.int32)

        def window(array):
            return jnp.take(array, chosen, axis=0).reshape(3 * CLIP, HEADS, HDIM)

        key_win = window(keys4)
        value_win = window(values4)
        ktan_win = window(ktan4)
        vtan_win = window(vtan4)
        query_clip = queries4[clip_index]
        qtan_clip = qtan4[clip_index]

        def one_head(head_index):
            return attend_head(jnp.take(query_clip, head_index, axis=1), jnp.take(qtan_clip, head_index, axis=1),
                               jnp.take(key_win, head_index, axis=1), jnp.take(value_win, head_index, axis=1),
                               jnp.take(ktan_win, head_index, axis=1), jnp.take(vtan_win, head_index, axis=1))

        head_out, head_tan = lax.map(one_head, jnp.arange(HEADS, dtype=jnp.int32))
        return jnp.transpose(head_out, (1, 0, 2)), jnp.transpose(head_tan, (1, 0, 2))

    clip_out, clip_tan = lax.map(one_clip, jnp.arange(CLIPS, dtype=jnp.int32))
    attended = clip_out.reshape(TOKENS, QW)
    attended_tangent = clip_tan.reshape(TOKENS, QW)
    weight_grad = lax.dot_general(cotangent, attended, (((0,), (0,)), ((), ())), preferred_element_type=jnp.float32)
    return attended, attended_tangent, weight_grad
```

```python
import functools
import math

import jax
import jax.numpy as jnp
from jax import lax
from jax.experimental import pallas as pl
from jax.experimental.pallas import tpu as pltpu
from jax.sharding import PartitionSpec as P

HDIM = 128
CLIP = 1024
NT = (((1,), (1,)), ((), ()))


def attend_rows(query, qtan, wk, wv, scale):
    f32 = jnp.float32
    hdim = query.shape[1]
    scores = lax.dot_general(query, wk[:, :hdim], NT, preferred_element_type=f32)
    both = jnp.concatenate([qtan, query], axis=1)
    score_tan = lax.dot_general(both, wk[...], NT, preferred_element_type=f32)
    row_max = jnp.max(scores, axis=1, keepdims=True)
    weights = jnp.exp2((scores - row_max) * (scale * math.log2(math.e)))
    inverse = 1.0 / jnp.sum(weights, axis=1, keepdims=True)
    mean = jnp.sum(weights * score_tan, axis=1, keepdims=True) * inverse
    low = weights.astype(jnp.bfloat16)
    tan_low = (weights * (score_tan - mean)).astype(jnp.bfloat16)
    first = jnp.dot(low, wv[...], preferred_element_type=f32)
    second = jnp.dot(tan_low, wv[:, :hdim], preferred_element_type=f32)
    out = first[:, :hdim] * inverse
    tan = (first[:, hdim:] + second * scale) * inverse
    return out.astype(jnp.bfloat16), tan.astype(jnp.bfloat16)


def attention_kernel(
    clips_here, slots, q, qt, k, v, kt, vt, pk, pv, pkt, pvt, out, tan, wk, wv
):
    within, block = pl.program_id(1), pl.program_id(2)

    @pl.when(block == 0)
    def _():
        def fill(place, own, slot):
            def put(a, b, c, d):
                rows = pl.ds(pl.multiple_of(slot * CLIP, CLIP), CLIP)
                at = pl.ds(place * CLIP, CLIP)
                wk[at, :HDIM] = a[rows, :]
                wk[at, HDIM:] = b[rows, :]
                wv[at, :HDIM] = c[rows, :]
                wv[at, HDIM:] = d[rows, :]

            if own:
                put(k, kt, v, vt)
            else:
                put(pk, pkt, pv, pvt)

        fill(0, True, within)
        for place in (1, 2):
            slot = slots[within * 2 + place - 1]

            @pl.when(slot < clips_here)
            def _():
                fill(place, False, slot)

            @pl.when(slot >= clips_here)
            def _():
                fill(place, True, slot - clips_here)

    out[...], tan[...] = attend_rows(q[...], qt[...], wk, wv, HDIM**-0.5)


def attention(slots, query, qtan, own, prev):
    rows, cols = query.shape
    clips_here = rows // CLIP
    block_rows = min(256, CLIP)
    blocks = CLIP // block_rows
    row_spec = pl.BlockSpec((block_rows, HDIM), lambda h, c, b, s: (c * blocks + b, h))
    all_spec = pl.BlockSpec((rows, HDIM), lambda h, c, b, s: (0, h))
    shape = jax.ShapeDtypeStruct((rows, cols), jnp.bfloat16)
    return pl.pallas_call(
        functools.partial(attention_kernel, clips_here),
        out_shape=(shape, shape),
        grid_spec=pltpu.PrefetchScalarGridSpec(
            num_scalar_prefetch=1,
            grid=(cols // HDIM, clips_here, blocks),
            in_specs=[row_spec] * 2 + [all_spec] * 8,
            out_specs=[row_spec] * 2,
            scratch_shapes=[
                pltpu.VMEM((3 * CLIP, 2 * HDIM), jnp.bfloat16),
                pltpu.VMEM((3 * CLIP, 2 * HDIM), jnp.bfloat16),
            ],
        ),
        compiler_params=pltpu.CompilerParams(vmem_limit_bytes=60 * 1024 * 1024),
        cost_estimate=pl.CostEstimate(
            flops=12 * rows * cols * 3 * CLIP,
            bytes_accessed=12 * rows * cols * 2,
            transcendentals=rows * cols // HDIM * 3 * CLIP,
        ),
    )(slots, query, qtan, *own, *prev)


def on_device(
    queries, key_rows, value_rows, query_tangent, key_tangent, value_tangent, partners, cotangent
):
    clip_count = lax.axis_size("clip")
    ring = [(i, (i + 1) % clip_count) for i in range(clip_count)]

    def to_heads(a):
        return lax.all_to_all(a, "head", split_axis=1, concat_axis=0, tiled=True)

    own = tuple(to_heads(a) for a in (key_rows, value_rows, key_tangent, value_tangent))
    prev = tuple(lax.ppermute(a, "clip", ring) for a in own)
    query_h, qtan_h = to_heads(queries), to_heads(query_tangent)
    clips_here = query_h.shape[0] // CLIP
    first_clip = lax.axis_index("clip") * clips_here
    mine = lax.dynamic_slice_in_dim(partners, first_clip, clips_here, 0)
    slots = ((mine - first_clip + clips_here) % (clips_here * clip_count)).reshape(-1)
    output_h, tangent_h = attention(slots, query_h, qtan_h, own, prev)
    partial_term = lax.dot_general(
        cotangent, output_h, (((0,), (0,)), ((), ())), preferred_element_type=jnp.float32
    )
    weight_grad = lax.psum_scatter(partial_term, "clip", scatter_dimension=0, tiled=True)

    def to_tokens(a):
        return lax.all_to_all(a, "head", split_axis=0, concat_axis=1, tiled=True)

    return (to_tokens(output_h), to_tokens(tangent_h), weight_grad)


def solution(mesh):
    tokens = P(("clip", "head"), None)
    return jax.shard_map(
        on_device,
        mesh=mesh,
        in_specs=(tokens,) * 6 + (P(), P("clip", None)),
        out_specs=(tokens, tokens, P("clip", "head")),
        check_vma=False,
    )
```
